512 devices in a mesh: prow: 16 (over y, x), pcol: 32 (over z, core).
Axes of the slice: x: 4, y: 4, z: 16, core: 2. Of those that a mesh axis runs over, the one named last changes fastest.
Arguments:
- schur: float32 [4, 16, 128, 2, 32, 128], P(None, 'prow', None, None, 'pcol'), may hold values from -0.0625 to 0.0625
- panel_inverse: float32 [2, 32, 128, 2, 16, 128], P(None, 'pcol', None, None, 'prow'), may hold values from -0.09375 to 0.09375
- coupling: float32 [4, 16, 128, 256], P(None, 'prow'), may hold values from -6 to 6
- zslab: float32 [4, 16, 128, 2, 32, 128], P(None, 'prow', None, None, 'pcol')
- targets: int32 [128], replicated, may hold values from 0 to 254
- pair_flags: int32 [128], replicated, may hold values 0 or 1
Outputs:
- eigenvectors: float32 [4, 16, 128, 128], P(None, 'prow', 'pcol')
The draws below stay inside these ranges and needn't reach their ends.
All inputs are finite; a program needn't handle non-finite values.
Results may differ from the reference program's by a relative error of at most 0.0001.
Values sent between devices are 32-bit elements; how exact they have to be, the bound alone decides.
No kernel may reach another device: no remote copies, remote signals or barrier semaphores. Data moves between devices by JAX's collectives and lax.ppermute only.
A program may use at most 64 MiB of HBM per device.

```python
import math
import jax
import jax.numpy as jnp
from jax import lax

BS = 128
NRHS = 128
WIN = 256
CBLK = 2
ZRB = 4
PW = 4096
RP = 2
K = 8192
RBLK = 4
ZROWS = 8192
N_PROW = 16
N_PCOL = 32


def draw_zslab(key, part):
    normal_key, scale_key = jax.random.split(jax.random.fold_in(key, 17))
    full_shape = (ZRB, N_PROW, BS, CBLK, N_PCOL, BS)
    entries = jax.random.normal(normal_key, full_shape, jnp.float32)
    spread = jax.random.uniform(scale_key, (ZRB, N_PROW, BS), jnp.float32)
    prow_frac = jnp.arange(N_PROW, dtype=jnp.float32) / (N_PROW - 1)
    share_frac = (jnp.arange(BS, dtype=jnp.int32) // (BS // N_PCOL)).astype(jnp.float32) / (N_PCOL - 1)
    exponent = 0.25 * prow_frac[None, :, None] + 0.25 * share_frac[None, None, :] + 0.5 * spread
    row_scale = jnp.power(10.0, exponent) / math.sqrt(K)
    return entries * row_scale[:, :, :, None, None, None]


def plant(array, stream_key, least, high):
    shape = array.shape
    place = [jax.random.randint(jax.random.fold_in(stream_key, axis), (), 0, shape[axis]) for axis in range(len(shape))]
    array = array.at[tuple(place)].set(least)
    longest = shape.index(max(shape))
    place[longest] = (place[longest] + 1) % shape[longest]
    return array.at[tuple(place)].set(high)


def block_scale(own_key, shape, cuts, low, top_value):
    def one(axis_at, shards_of):
        heights = jax.random.uniform(jax.random.fold_in(jax.random.fold_in(own_key, 6), axis_at), (shards_of,), jnp.float32, low / len(cuts), top_value / len(cuts))
        return jnp.repeat(jnp.exp(heights), shape[axis_at] // shards_of).reshape((-1,) + (1,) * (len(shape) - axis_at - 1))

    loudness = one(*cuts[0])
    for cut in cuts[1:]:
        loudness = loudness * one(*cut)
    return loudness


def normal_values(stream_key, extent, scale, reach, cuts=(), kind=jnp.bfloat16):
    result = jax.random.normal(stream_key, extent, jnp.float32) * scale
    if len(cuts) > 0:
        result = block_scale(stream_key, extent, cuts, -0.22, 0.18) * result
    return jnp.clip(result, min=-reach, max=reach).astype(kind)


def setup_inputs(seed: int = 0) -> dict:
    key_list = jax.random.split(jax.random.key(seed), 7)
    schur = normal_values(key_list[0], (RBLK, N_PROW, BS, CBLK, N_PCOL, BS), K ** -0.5, 0.0625, ((1, 16), (4, 32)), jnp.float32)
    panel_inverse = normal_values(key_list[1], (CBLK, N_PCOL, BS, RP, N_PROW, BS), PW ** -0.5, 0.09375, ((1, 32), (4, 16)), jnp.float32)
    coupling = normal_values(key_list[2], (RBLK, N_PROW, BS, WIN), 1.0, 6.0, ((1, 16),), jnp.float32)
    zslab = draw_zslab(jax.random.fold_in(key_list[6], 71), 0)
    targets = plant(jax.random.randint(key_list[4], (NRHS,), 0, WIN - 1), jax.random.fold_in(key_list[4], 1), 0, (WIN - 1) - 1).astype(jnp.int32)
    pair_flags = plant((jax.random.randint(key_list[5], (NRHS,), 0, 2) < 1).astype(jnp.int32), jax.random.fold_in(key_list[5], 1), 0, 1)
    return dict(schur=schur, panel_inverse=panel_inverse, coupling=coupling, zslab=zslab, targets=targets, pair_flags=pair_flags)


EPSILON = 1e-06

def reference(schur, panel_inverse, coupling, zslab, targets, pair_flags):
    triangle = schur.reshape(K, K)
    columns = jnp.arange(WIN, dtype=jnp.int32)[:, None]
    selection = (columns == targets[None, :]).astype(jnp.float32) + pair_flags[None, :].astype(jnp.float32) * (columns == targets[None, :] + 1).astype(jnp.float32)
    right_side = -jnp.dot(coupling.reshape(K, WIN), selection, precision=lax.Precision.HIGHEST)
    inverse = panel_inverse.reshape(CBLK, PW, PW)
    pieces = [None] * CBLK
    for panel_index in reversed(range(CBLK)):
        residual = right_side[panel_index * PW:(panel_index + 1) * PW]
        if panel_index < CBLK - 1:
            later_rows = jnp.concatenate(pieces[panel_index + 1:], axis=0)
            residual = residual - jnp.dot(triangle[panel_index * PW:(panel_index + 1) * PW, (panel_index + 1) * PW:], later_rows, precision=lax.Precision.HIGHEST)
        pieces[panel_index] = jnp.dot(inverse[panel_index], residual, precision=lax.Precision.HIGHEST)
    vectors = jnp.concatenate(pieces, axis=0)
    transformed = jnp.dot(zslab.reshape(ZROWS, K), vectors, precision=lax.Precision.HIGHEST)
    column_norms = jnp.sqrt(lax.optimization_barrier(jnp.mean(transformed * transformed, axis=0)) + EPSILON)
    return (transformed / column_norms[None, :]).reshape(ZRB, N_PROW, BS, NRHS)
```

```python
import jax
import jax.numpy as jnp
from jax import lax
from jax.sharding import Mesh
from jax.sharding import PartitionSpec as P

PROW = ("prow_0", "prow_1")
PCOL = ("pcol_0", "pcol_1")
LINE = "pcol_0"
CORE = "pcol_1"


EPSILON = 1e-06


def product(left, right):
    return jnp.dot(left, right, precision=lax.Precision.HIGHEST)


def packed(value):
    rows = value.shape[0] // 2
    return jnp.concatenate([value[:rows], value[rows:]], axis=1)


def unpacked(value):
    lanes = value.shape[1] // 2
    return jnp.concatenate([value[:, :lanes], value[:, lanes:]], axis=0)


def from_everyone(value, axis):
    size = lax.axis_size(axis)
    return lax.all_to_all(
        jnp.broadcast_to(value[None], (size, *value.shape)), axis, 0, 0, tiled=True
    )


def over_copies(value, axis):
    return jnp.sum(from_everyone(value, axis), axis=0)


def shards(schur, panel_inverse, coupling, zslab, targets, pair_flags):
    block_size = schur.shape[2]
    row_blocks = schur.shape[0]
    window = coupling.shape[3]
    zrow_blocks = zslab.shape[0]
    half_blocks = row_blocks // 2
    panel_part = panel_inverse.shape[3] * block_size
    cores = lax.axis_size(CORE)
    line = lax.axis_size(LINE)
    share = targets.shape[0] // cores
    core = lax.axis_index(CORE)

    inverse = lax.all_gather(panel_inverse.reshape(2, block_size, panel_part), CORE, axis=1, tiled=True)
    strip = coupling.reshape(row_blocks * block_size, window)
    triangle = lax.all_gather(
        schur[:half_blocks, 0, :, 1, 0, :].reshape(half_blocks * block_size, block_size),
        CORE, axis=1, tiled=True,
    )
    z_rows = [
        lax.all_gather(
            zslab[:, 0, :, j, 0, :].reshape(zrow_blocks * block_size, block_size), CORE, axis=1, tiled=True
        )
        for j in range(2)
    ]

    own_targets = lax.dynamic_slice_in_dim(targets, core * share, share)
    own_flags = lax.dynamic_slice_in_dim(pair_flags, core * share, share)
    columns = jnp.arange(window, dtype=jnp.int32)[:, None]
    selection = (columns == own_targets[None, :]).astype(jnp.float32) + own_flags[None, :].astype(
        jnp.float32
    ) * (columns == own_targets[None, :] + 1).astype(jnp.float32)
    right_side = -product(strip, selection)
    early, late = right_side[:panel_part], right_side[panel_part:]

    later = unpacked(over_copies(packed(product(inverse[1], late)), PROW))
    partial_value = packed(product(triangle, later))
    pieces = lax.all_to_all(partial_value.reshape(line, -1, partial_value.shape[1]), LINE, 0, 0, tiled=True)
    summed = from_everyone(jnp.sum(pieces, axis=0), LINE).reshape(partial_value.shape)
    residual = early - unpacked(summed)
    sooner = unpacked(over_copies(packed(product(inverse[0], residual)), PROW))
    transformed = packed(product(z_rows[0], sooner) + product(z_rows[1], later))
    lanes = transformed.shape[1]
    stacked = jnp.moveaxis(
        transformed.reshape(zrow_blocks // 2, line, block_size // line, lanes), 1, 0
    )
    owned = jnp.sum(lax.all_to_all(stacked, LINE, 0, 0, tiled=True), axis=0)
    both = lax.all_gather(owned, CORE, axis=0, tiled=False)
    squares = jnp.sum(both * both, axis=(1, 2)).reshape(cores, 2, share).sum(axis=1).reshape(1, cores * share)
    squares = over_copies(over_copies(squares, LINE), PROW)
    total_rows = zrow_blocks * block_size * lax.axis_size(PROW)
    divisor = jnp.sqrt(squares / total_rows + EPSILON)
    rows = block_size // line // cores
    mine = lax.dynamic_slice_in_dim(both, core * rows, rows, axis=2)
    mine = mine.reshape(cores, zrow_blocks // 2, rows, 2, share).transpose(3, 1, 2, 0, 4)
    mine = mine.reshape(zrow_blocks, 1, rows, cores * share)
    return mine / divisor[None, None]


def solution(mesh):
    split = Mesh(mesh.devices.reshape(4, 4, 16, 2), ("prow_0", "prow_1", "pcol_0", "pcol_1"))
    placed = (
        P(None, PROW, None, None, PCOL, None),
        P(None, PCOL, None, None, PROW, None),
        P(None, PROW, None, None),
        P(None, PROW, None, None, PCOL, None),
        P(),
        P(),
    )
    return jax.shard_map(
        shards, mesh=split, in_specs=placed, out_specs=P(None, PROW, PCOL, None), check_vma=False
    )
```

```python
import functools

import jax
import jax.numpy as jnp
from jax import lax
from jax.experimental import pallas as pl
from jax.experimental.pallas import tpu as pltpu
from jax.sharding import Mesh
from jax.sharding import PartitionSpec as P

PROW = ("prow_0", "prow_1")
PCOL = ("pcol_0", "pcol_1")
LINE = "pcol_0"
CORE = "pcol_1"


EPSILON = 1e-06


def product(left, right):
    return jnp.dot(left, right, precision=lax.Precision.HIGHEST, preferred_element_type=jnp.float32)


def exchanged(value, axis):
    return lax.all_to_all(value, axis, 0, 0, tiled=True)


def first_half(shape):
    return lax.broadcasted_iota(jnp.int32, shape, 1) < shape[1] // 2


def turned(value):
    return pltpu.roll(value, value.shape[1] // 2, 1)


def doubled(value):
    left, other = first_half(value.shape), turned(value)
    return jnp.where(left, value, other), jnp.where(left, other, value)


def merged(low, high):
    return jnp.where(first_half(low.shape), low, high)


def strided(ref, core, start, count, step):
    return ref[core, pl.ds(start, count, stride=step), :]


def begin(core_ref, targets_ref, flags_ref, strip_ref, inverse_ref, sent_ref, early_ref, *, block):
    window = strip_ref.shape[1]
    panel = strip_ref.shape[0] // 2
    parts = panel // block
    lanes = targets_ref.shape[1]
    home = first_half((1, lanes)) == (core_ref[0] == 0)
    targets = jnp.where(home, targets_ref[...], turned(targets_ref[...]))
    flags = jnp.where(home, flags_ref[...], turned(flags_ref[...])).astype(jnp.float32)
    columns = lax.broadcasted_iota(jnp.int32, (window, lanes), 0)
    selection = (columns == targets).astype(jnp.float32) + flags * (columns == targets + 1).astype(
        jnp.float32
    )
    late = -product(strip_ref[panel:, :], selection)
    applied = []
    for core in range(2):
        applied.append(
            sum(
                product(
                    strided(inverse_ref, core, parts * block + part, block, parts),
                    late[part * block : (part + 1) * block],
                )
                for part in range(parts)
            )
        )
    out = merged(*applied)
    for peer in range(sent_ref.shape[0]):
        sent_ref[peer] = out
    early_ref[...] = -product(strip_ref[:panel, :], selection)


def coupled(pieces_ref, triangle_ref, sent_ref, later_ref, *, block):
    later = jnp.sum(pieces_ref[...], axis=0)
    later_ref[...] = later
    halves = doubled(later)
    values = []
    for part in range(2):
        values.append(
            sum(
                product(strided(triangle_ref, core, part * 2 * block + 1, block, 2), halves[core])
                for core in range(2)
            )
        )
    sent_ref[...] = merged(*values)


def solved(summed_ref, early_ref, inverse_ref, sent_ref, *, block):
    halves = doubled(summed_ref[...])
    parts = early_ref.shape[0] // block
    residual = [early_ref[part * block : (part + 1) * block, :] - halves[part] for part in range(parts)]
    applied = []
    for core in range(2):
        applied.append(
            sum(
                product(strided(inverse_ref, core, part, block, parts), residual[part])
                for part in range(parts)
            )
        )
    out = merged(*applied)
    for peer in range(sent_ref.shape[0]):
        sent_ref[peer] = out


def carried(pieces_ref, later_ref, low_ref, high_ref, sent_ref, *, block):
    sooner = doubled(jnp.sum(pieces_ref[...], axis=0))
    later = doubled(later_ref[...])
    values = []
    for ref in (low_ref, high_ref):
        rows = ref.shape[1] // 2
        values.append(
            sum(
                product(strided(ref, core, 0, rows, 2), sooner[core])
                + product(strided(ref, core, 1, rows, 2), later[core])
                for core in range(2)
            )
        )
    out = merged(*values)
    peers, stacks, rows, lanes = sent_ref.shape
    for stack in range(stacks):
        sent_ref[:, stack] = out[stack * block : (stack + 1) * block].reshape(peers, rows, lanes)


def squared(both_ref, sent_ref):
    both = both_ref[...]
    cores, stacks, rows, lanes = both.shape
    squares = jnp.sum((both * both).reshape(cores, stacks * rows, lanes), axis=1)
    squares = squares + turned(squares)
    out = merged(squares[0:1], squares[1:2])
    sent_ref[...] = jnp.broadcast_to(out[None], sent_ref.shape)


def again(pieces_ref, sent_ref):
    sent_ref[...] = jnp.broadcast_to(jnp.sum(pieces_ref[...], axis=0, keepdims=True), sent_ref.shape)


def finished(core_ref, both_ref, pieces_ref, out_ref, *, total):
    squares = jnp.sum(pieces_ref[...], axis=0)
    divisor = jnp.sqrt(squares / total + EPSILON)
    stacks = both_ref.shape[1]
    rows = out_ref.shape[2]
    for stack in range(stacks):
        low = both_ref[0, stack]
        high = both_ref[1, stack]
        for side, value in enumerate((merged(low, turned(high)), merged(turned(low), high))):
            value = value / divisor
            own = jnp.where(core_ref[0] == 0, value[:rows], value[rows:])
            out_ref[side * stacks + stack, 0] = own


LIMIT = 12 * 2**20
SCALAR = pl.BlockSpec(memory_space=pltpu.SMEM)
LOCAL = pl.BlockSpec(memory_space=pltpu.VMEM)


def kernel(body, shapes, *args, scalars=0, **settings):
    outs = [jax.ShapeDtypeStruct(shape, jnp.float32) for shape in shapes]
    single = len(outs) == 1
    return pl.pallas_call(
        functools.partial(body, **settings),
        out_shape=outs[0] if single else outs,
        in_specs=[SCALAR] * scalars + [LOCAL] * (len(args) - scalars),
        out_specs=LOCAL if single else [LOCAL] * len(outs),
        name=body.__name__,
        compiler_params=pltpu.CompilerParams(vmem_limit_bytes=LIMIT),
    )(*args)


def shards(schur, panel_inverse, coupling, zslab, targets, pair_flags):
    block = schur.shape[2]
    row_blocks = schur.shape[0]
    window = coupling.shape[3]
    zrow_blocks = zslab.shape[0]
    count = targets.shape[0]
    line = lax.axis_size(LINE)
    peers = lax.axis_size(PROW)
    panel = panel_inverse.shape[3] * block
    core = lax.axis_index(CORE).astype(jnp.int32).reshape(1)

    inverse = lax.all_gather(panel_inverse.reshape(-1, block), CORE)
    strip = coupling.reshape(row_blocks * block, window)
    sent, early = kernel(
        begin,
        [(peers, block, count), (panel, count)],
        core, targets.reshape(1, count), pair_flags.reshape(1, count), strip, inverse,
        scalars=1, block=block,
    )
    pieces = exchanged(sent, PROW)
    triangle = lax.all_gather(schur[: row_blocks // 2].reshape(-1, block), CORE)
    low = lax.all_gather(zslab[: zrow_blocks // 2].reshape(-1, block), CORE)
    high = lax.all_gather(zslab[zrow_blocks // 2 :].reshape(-1, block), CORE)
    pieces, triangle, low, high = lax.optimization_barrier((pieces, triangle, low, high))
    partial_value, later = kernel(
        coupled, [(block, count), (block, count)], pieces, triangle, block=block
    )
    parts = exchanged(partial_value.reshape(line, -1, count), LINE)
    mine = jnp.sum(parts, axis=0)
    summed = exchanged(jnp.broadcast_to(mine[None], (line, *mine.shape)), LINE).reshape(block, count)
    sent = kernel(solved, [(peers, block, count)], summed, early, inverse, block=block)
    pieces = exchanged(sent, PROW)
    stacked = kernel(
        carried,
        [(line, zrow_blocks // 2, block // line, count)],
        pieces, later, low, high, block=block,
    )
    owned = jnp.sum(exchanged(stacked, LINE), axis=0)
    both = lax.all_gather(owned, CORE)
    squares = exchanged(kernel(squared, [(line, 1, count)], both), LINE)
    squares = exchanged(kernel(again, [(peers, 1, count)], squares), PROW)
    total = zrow_blocks * block * peers
    rows = block // line // lax.axis_size(CORE)
    return kernel(
        finished, [(zrow_blocks, 1, rows, count)], core, both, squares, scalars=1, total=total
    )


def solution(mesh):
    split = Mesh(mesh.devices.reshape(4, 4, 16, 2), ("prow_0", "prow_1", "pcol_0", "pcol_1"))
    placed = (
        P(None, PROW, None, None, PCOL, None),
        P(None, PCOL, None, None, PROW, None),
        P(None, PROW, None, None),
        P(None, PROW, None, None, PCOL, None),
        P(),
        P(),
    )
    return jax.shard_map(
        shards, mesh=split, in_specs=placed, out_specs=P(None, PROW, PCOL, None), check_vma=False
    )
```

```python
import functools

import jax
import jax.numpy as jnp
from jax import lax
from jax.experimental import pallas as pl
from jax.experimental.pallas import tpu as pltpu
from jax.sharding import Mesh
from jax.sharding import PartitionSpec as P

PROW = ("prow_0", "prow_1")
PCOL = ("pcol_0", "pcol_1")
LINE = "pcol_0"
CORE = "pcol_1"


EPSILON = 1e-06


def product(left, right):
    return jnp.dot(left, right, precision=lax.Precision.HIGHEST, preferred_element_type=jnp.float32)


def exchanged(value, axis):
    return lax.all_to_all(value, axis, 0, 0, tiled=True)


def first_half(shape):
    return lax.broadcasted_iota(jnp.int32, shape, 1) < shape[1] // 2


def turned(value):
    return pltpu.roll(value, value.shape[1] // 2, 1)


def doubled(value):
    left, other = first_half(value.shape), turned(value)
    return jnp.where(left, value, other), jnp.where(left, other, value)


def merged(low, high):
    return jnp.where(first_half(low.shape), low, high)


def strided(ref, core, start, count, step):
    return ref[core, pl.ds(start, count, stride=step), :]


def selected(targets_ref, flags_ref, window):
    lanes = targets_ref.shape[1]
    targets = targets_ref[...]
    columns = lax.broadcasted_iota(jnp.int32, (window, lanes), 0)
    flags = flags_ref[...].astype(jnp.float32)
    chosen = (columns == targets).astype(jnp.float32) + flags * (columns == targets + 1).astype(
        jnp.float32
    )
    return chosen.astype(jnp.bfloat16)


def thirds(value):
    high = value.astype(jnp.bfloat16)
    rest = value - high.astype(jnp.float32)
    middle = rest.astype(jnp.bfloat16)
    low = (rest - middle.astype(jnp.float32)).astype(jnp.bfloat16)
    return high, middle, low


def picked(parts, chosen):
    return sum(jnp.dot(part, chosen, preferred_element_type=jnp.float32) for part in reversed(parts))


def across(value, core):
    left, right = doubled(value)
    return jnp.where(core == 0, left, right)


def begin(
    strip_hbm, targets_hbm, flags_hbm, inverse_hbm,
    sent_ref, strip_ref, targets_ref, flags_ref, inverse_ref, sems,
):
    panel, window = strip_ref.shape
    block = sent_ref.shape[1]
    half = inverse_ref.shape[1]
    copies = [
        pltpu.make_async_copy(strip_hbm.at[pl.ds(panel, panel)], strip_ref, sems.at[0]),
        pltpu.make_async_copy(targets_hbm, targets_ref, sems.at[1]),
        pltpu.make_async_copy(flags_hbm, flags_ref, sems.at[2]),
        pltpu.make_async_copy(inverse_hbm.at[pl.ds(half, half)], inverse_ref.at[0], sems.at[3]),
    ]
    for copy in copies:
        copy.start()
    copies[1].wait()
    copies[2].wait()
    chosen = selected(targets_ref, flags_ref, window)
    copies[0].wait()
    late = -picked(thirds(strip_ref[...]), chosen)
    copies[3].wait()
    out = product(columns_of(inverse_ref, 0, 0, block), late)
    for peer in range(sent_ref.shape[0]):
        sent_ref[peer] = out


def columns_of(ref, core, start, count):
    return jnp.concatenate(
        [strided(ref, core, start, count, 2), strided(ref, core, start + 1, count, 2)], axis=1
    )


def opening(core_ref, targets_ref, flags_ref, strip_ref, early_ref):
    panel = strip_ref.shape[0] // 2
    chosen = selected(targets_ref, flags_ref, strip_ref.shape[1])
    early_ref[...] = across(-picked(thirds(strip_ref[:panel, :]), chosen), core_ref[0])


def coupled(core_ref, solved_ref, triangle_ref, sent_ref, later_ref, *, block):
    halves = [across(solved_ref[core], core_ref[0]) for core in range(2)]
    later_ref[...] = merged(*halves)
    both = jnp.concatenate(halves, axis=0)
    values = []
    for part in range(2):
        blocks = [strided(triangle_ref, core, part * 2 * block + 1, block, 2) for core in range(2)]
        values.append(product(jnp.concatenate(blocks, axis=1), both))
    sent_ref[...] = merged(*values)


def solved(summed_ref, early_ref, inverse_ref, sent_ref, *, block):
    residual = early_ref[...] - jnp.concatenate(doubled(summed_ref[...]), axis=0)
    out = merged(*[product(columns_of(inverse_ref, core, 0, block), residual) for core in range(2)])
    for peer in range(sent_ref.shape[0]):
        sent_ref[peer] = out


def carried(pieces_ref, later_ref, low_ref, high_ref, sent_ref, *, block):
    sooner = doubled(jnp.sum(pieces_ref[...], axis=0))
    later = doubled(later_ref[...])
    known = [jnp.concatenate([sooner[core], later[core]], axis=0) for core in range(2)]
    values = []
    for ref in (low_ref, high_ref):
        rows = ref.shape[1] // 2
        values.append(sum(product(columns_of(ref, core, 0, rows), known[core]) for core in range(2)))
    out = merged(*values)
    peers, stacks, rows, lanes = sent_ref.shape
    for stack in range(stacks):
        sent_ref[:, stack] = out[stack * block : (stack + 1) * block].reshape(peers, rows, lanes)


def squared(both_ref, sent_ref):
    both = both_ref[...]
    cores, stacks, rows, lanes = both.shape
    squares = jnp.sum((both * both).reshape(cores, stacks * rows, lanes), axis=1)
    squares = squares + turned(squares)
    out = merged(squares[0:1], squares[1:2])
    sent_ref[...] = jnp.broadcast_to(out[None], sent_ref.shape)


def again(pieces_ref, sent_ref):
    sent_ref[...] = jnp.broadcast_to(jnp.sum(pieces_ref[...], axis=0, keepdims=True), sent_ref.shape)


def finished(core_ref, both_ref, pieces_ref, out_ref, *, total):
    squares = jnp.sum(pieces_ref[...], axis=0)
    divisor = jnp.sqrt(squares / total + EPSILON)
    stacks = both_ref.shape[1]
    rows = out_ref.shape[2]
    for stack in range(stacks):
        low = both_ref[0, stack]
        high = both_ref[1, stack]
        for side, value in enumerate((merged(low, turned(high)), merged(turned(low), high))):
            value = value / divisor
            own = jnp.where(core_ref[0] == 0, value[:rows], value[rows:])
            out_ref[side * stacks + stack, 0] = own


LIMIT = 12 * 2**20
SCALAR = pl.BlockSpec(memory_space=pltpu.SMEM)
LOCAL = pl.BlockSpec(memory_space=pltpu.VMEM)
REMOTE = pl.BlockSpec(memory_space=pltpu.HBM)


def kernel(body, shapes, *args, scalars=0, distant=0, scratch=(), **settings):
    outs = [jax.ShapeDtypeStruct(shape, jnp.float32) for shape in shapes]
    single = len(outs) == 1
    return pl.pallas_call(
        functools.partial(body, **settings),
        out_shape=outs[0] if single else outs,
        in_specs=[SCALAR] * scalars + [LOCAL] * (len(args) - scalars - distant) + [REMOTE] * distant,
        out_specs=LOCAL if single else [LOCAL] * len(outs),
        scratch_shapes=list(scratch),
        name=body.__name__,
        compiler_params=pltpu.CompilerParams(vmem_limit_bytes=LIMIT),
    )(*args)


def shards(schur, panel_inverse, coupling, zslab, targets, pair_flags):
    block = schur.shape[2]
    row_blocks = schur.shape[0]
    window = coupling.shape[3]
    zrow_blocks = zslab.shape[0]
    count = targets.shape[0]
    line = lax.axis_size(LINE)
    peers = lax.axis_size(PROW)
    panel = panel_inverse.shape[3] * block
    core = lax.axis_index(CORE).astype(jnp.int32).reshape(1)

    strip = coupling.reshape(row_blocks * block, window)
    wanted = targets.reshape(1, count)
    paired = pair_flags.reshape(1, count)
    own_inverse = panel_inverse.reshape(-1, block)
    sent = kernel(
        begin, [(peers, block, count)],
        *[pltpu.with_memory_space_constraint(a, pltpu.HBM) for a in (strip, wanted, paired, own_inverse)],
        distant=4,
        scratch=(
            pltpu.VMEM((panel, window), jnp.float32),
            pltpu.VMEM((1, count), jnp.int32),
            pltpu.VMEM((1, count), jnp.int32),
            pltpu.VMEM((1, panel, block), jnp.float32),
            pltpu.SemaphoreType.DMA((4,)),
        ),
    )
    pieces = exchanged(sent, PROW)
    early = kernel(opening, [(panel, count)], core, wanted, paired, strip, scalars=1)
    inverse = lax.all_gather(panel_inverse[0].reshape(-1, block), CORE)
    triangle = lax.all_gather(schur[: row_blocks // 2].reshape(-1, block), CORE)
    low = lax.all_gather(zslab[: zrow_blocks // 2].reshape(-1, block), CORE)
    high = lax.all_gather(zslab[zrow_blocks // 2 :].reshape(-1, block), CORE)
    pieces, early, inverse, triangle, low, high = lax.optimization_barrier(
        (pieces, early, inverse, triangle, low, high)
    )
    whole = lax.all_gather(jnp.sum(pieces, axis=0), CORE)
    partial_value, later = kernel(
        coupled, [(block, count), (block, count)], core, whole, triangle, scalars=1, block=block
    )
    parts = exchanged(partial_value.reshape(line, -1, count), LINE)
    mine = jnp.sum(parts, axis=0)
    summed = exchanged(jnp.broadcast_to(mine[None], (line, *mine.shape)), LINE).reshape(block, count)
    sent = kernel(solved, [(peers, block, count)], summed, early, inverse, block=block)
    pieces = exchanged(sent, PROW)
    stacked = kernel(
        carried,
        [(line, zrow_blocks // 2, block // line, count)],
        pieces, later, low, high, block=block,
    )
    owned = jnp.sum(exchanged(stacked, LINE), axis=0)
    both = lax.all_gather(owned, CORE)
    squares = exchanged(kernel(squared, [(line, 1, count)], both), LINE)
    squares = exchanged(kernel(again, [(peers, 1, count)], squares), PROW)
    total = zrow_blocks * block * peers
    rows = block // line // lax.axis_size(CORE)
    return kernel(
        finished, [(zrow_blocks, 1, rows, count)], core, both, squares, scalars=1, total=total
    )


def solution(mesh):
    split = Mesh(mesh.devices.reshape(4, 4, 16, 2), ("prow_0", "prow_1", "pcol_0", "pcol_1"))
    placed = (
        P(None, PROW, None, None, PCOL, None),
        P(None, PCOL, None, None, PROW, None),
        P(None, PROW, None, None),
        P(None, PROW, None, None, PCOL, None),
        P(),
        P(),
    )
    return jax.shard_map(
        shards, mesh=split, in_specs=placed, out_specs=P(None, PROW, PCOL, None), check_vma=False
    )
```

```python
import functools

import jax
import jax.numpy as jnp
from jax import lax
from jax.experimental import pallas as pl
from jax.experimental.pallas import tpu as pltpu
from jax.sharding import Mesh
from jax.sharding import PartitionSpec as P

ROWS = ("prow_0", "prow_1", "prow_2", "prow_3")
LINE = "pcol_0"
CORE = "pcol_1"
PCOL = (LINE, CORE)


EPSILON = 1e-06

FIRST = {"prow_0": 1, "prow_1": 0, "prow_2": 1, "prow_3": 0, "pcol_0": 8, "pcol_1": 0}


def product(left, right):
    return jnp.dot(left, right, precision=lax.Precision.HIGHEST, preferred_element_type=jnp.float32)


def in_turn(first, sizes):
    order = [0]
    for start, size in zip(first, sizes, strict=True):
        order = [place * size + (start + step) % size for place in order for step in range(size)]
    return [order]


def exchanged(value, axis):
    names = (axis,) if isinstance(axis, str) else axis
    order = in_turn([FIRST[name] for name in names], [lax.axis_size(name) for name in names])
    return lax.all_to_all(value, axis, 0, 0, tiled=True, axis_index_groups=order)


def from_everyone(value, axis):
    size = lax.axis_size(axis)
    return exchanged(jnp.broadcast_to(value[None], (size, *value.shape)), axis)


def in_pairs(value, near, others):
    return from_everyone(jnp.sum(lax.all_gather(value, near), axis=0), others)


def first_half(shape):
    return lax.broadcasted_iota(jnp.int32, shape, 1) < shape[1] // 2


def turned(value):
    return pltpu.roll(value, value.shape[1] // 2, 1)


def doubled(value):
    left, other = first_half(value.shape), turned(value)
    return jnp.where(left, value, other), jnp.where(left, other, value)


def merged(low, high):
    return jnp.where(first_half(low.shape), low, high)


def strided(ref, core, start, count, step):
    return ref[core, pl.ds(start, count, stride=step), :]


def selected(targets_ref, flags_ref, window):
    lanes = targets_ref.shape[1]
    targets = targets_ref[...]
    columns = lax.broadcasted_iota(jnp.int32, (window, lanes), 0)
    flags = flags_ref[...].astype(jnp.float32)
    chosen = (columns == targets).astype(jnp.float32) + flags * (columns == targets + 1).astype(
        jnp.float32
    )
    return chosen.astype(jnp.bfloat16)


def thirds(value):
    high = value.astype(jnp.bfloat16)
    rest = value - high.astype(jnp.float32)
    middle = rest.astype(jnp.bfloat16)
    low = (rest - middle.astype(jnp.float32)).astype(jnp.bfloat16)
    return high, middle, low


def picked(parts, chosen):
    return sum(jnp.dot(part, chosen, preferred_element_type=jnp.float32) for part in reversed(parts))


def across(value, core):
    left, right = doubled(value)
    return jnp.where(core == 0, left, right)


def begin(
    strip_hbm, targets_hbm, flags_hbm, inverse_hbm,
    sent_ref, strip_ref, targets_ref, flags_ref, inverse_ref, sems,
):
    panel, window = strip_ref.shape
    block = sent_ref.shape[1]
    half = inverse_ref.shape[1]
    copies = [
        pltpu.make_async_copy(strip_hbm.at[pl.ds(panel, panel)], strip_ref, sems.at[0]),
        pltpu.make_async_copy(targets_hbm, targets_ref, sems.at[1]),
        pltpu.make_async_copy(flags_hbm, flags_ref, sems.at[2]),
        pltpu.make_async_copy(inverse_hbm.at[pl.ds(half, half)], inverse_ref.at[0], sems.at[3]),
    ]
    for copy in copies:
        copy.start()
    copies[1].wait()
    copies[2].wait()
    chosen = selected(targets_ref, flags_ref, window)
    copies[0].wait()
    late = -picked(thirds(strip_ref[...]), chosen)
    copies[3].wait()
    out = product(columns_of(inverse_ref, 0, 0, block), late)
    for peer in range(sent_ref.shape[0]):
        sent_ref[peer] = out


def columns_of(ref, core, start, count):
    return jnp.concatenate(
        [strided(ref, core, start, count, 2), strided(ref, core, start + 1, count, 2)], axis=1
    )


def opening(core_ref, targets_ref, flags_ref, strip_ref, early_ref):
    panel = strip_ref.shape[0] // 2
    chosen = selected(targets_ref, flags_ref, strip_ref.shape[1])
    early_ref[...] = across(-picked(thirds(strip_ref[:panel, :]), chosen), core_ref[0])


def coupled(core_ref, solved_ref, triangle_ref, sent_ref, later_ref, *, block):
    halves = [across(solved_ref[core], core_ref[0]) for core in range(2)]
    later_ref[...] = merged(*halves)
    both = jnp.concatenate(halves, axis=0)
    values = []
    for part in range(2):
        blocks = [strided(triangle_ref, core, part * 2 * block + 1, block, 2) for core in range(2)]
        values.append(product(jnp.concatenate(blocks, axis=1), both))
    sent_ref[...] = merged(*values)


def solved(summed_ref, early_ref, inverse_ref, sent_ref, *, block):
    residual = early_ref[...] - jnp.concatenate(doubled(summed_ref[...]), axis=0)
    sent_ref[...] = merged(
        *[product(columns_of(inverse_ref, core, 0, block), residual) for core in range(2)]
    )


def carried(pieces_ref, later_ref, low_ref, high_ref, sent_ref, *, block):
    sooner = doubled(jnp.sum(pieces_ref[...], axis=0))
    later = doubled(later_ref[...])
    known = [jnp.concatenate([sooner[core], later[core]], axis=0) for core in range(2)]
    values = []
    for ref in (low_ref, high_ref):
        rows = ref.shape[1] // 2
        values.append(sum(product(columns_of(ref, core, 0, rows), known[core]) for core in range(2)))
    out = merged(*values)
    peers, stacks, rows, lanes = sent_ref.shape
    first = FIRST[LINE]
    for stack in range(stacks):
        shares = out[stack * block : (stack + 1) * block].reshape(peers, rows, lanes)
        sent_ref[: peers - first, stack] = shares[first:]
        if first:
            sent_ref[peers - first :, stack] = shares[:first]


def squared(both_ref, sent_ref):
    both = both_ref[...]
    cores, stacks, rows, lanes = both.shape
    squares = jnp.sum((both * both).reshape(cores, stacks * rows, lanes), axis=1)
    squares = squares + turned(squares)
    out = merged(squares[0:1], squares[1:2])
    sent_ref[...] = jnp.broadcast_to(out[None], sent_ref.shape)


def again(pieces_ref, sent_ref):
    sent_ref[...] = jnp.broadcast_to(jnp.sum(pieces_ref[...], axis=0, keepdims=True), sent_ref.shape)


def finished(core_ref, both_ref, pieces_ref, out_ref, *, total):
    squares = jnp.sum(pieces_ref[...], axis=0)
    divisor = jnp.sqrt(squares / total + EPSILON)
    stacks = both_ref.shape[1]
    rows = out_ref.shape[2]
    for stack in range(stacks):
        low = both_ref[0, stack]
        high = both_ref[1, stack]
        for side, value in enumerate((merged(low, turned(high)), merged(turned(low), high))):
            value = value / divisor
            own = jnp.where(core_ref[0] == 0, value[:rows], value[rows:])
            out_ref[side * stacks + stack, 0] = own


LIMIT = 12 * 2**20
SCALAR = pl.BlockSpec(memory_space=pltpu.SMEM)
LOCAL = pl.BlockSpec(memory_space=pltpu.VMEM)
REMOTE = pl.BlockSpec(memory_space=pltpu.HBM)


def kernel(body, shapes, *args, scalars=0, distant=0, scratch=(), **settings):
    outs = [jax.ShapeDtypeStruct(shape, jnp.float32) for shape in shapes]
    single = len(outs) == 1
    return pl.pallas_call(
        functools.partial(body, **settings),
        out_shape=outs[0] if single else outs,
        in_specs=[SCALAR] * scalars + [LOCAL] * (len(args) - scalars - distant) + [REMOTE] * distant,
        out_specs=LOCAL if single else [LOCAL] * len(outs),
        scratch_shapes=list(scratch),
        name=body.__name__,
        compiler_params=pltpu.CompilerParams(vmem_limit_bytes=LIMIT),
    )(*args)


def shards(schur, panel_inverse, coupling, zslab, targets, pair_flags):
    block = schur.shape[2]
    row_blocks = schur.shape[0]
    window = coupling.shape[3]
    zrow_blocks = zslab.shape[0]
    count = targets.shape[0]
    line = lax.axis_size(LINE)
    peers = lax.axis_size(ROWS)
    panel = panel_inverse.shape[3] * block
    core = lax.axis_index(CORE).astype(jnp.int32).reshape(1)

    strip = coupling.reshape(row_blocks * block, window)
    wanted = targets.reshape(1, count)
    paired = pair_flags.reshape(1, count)
    own_inverse = panel_inverse.reshape(-1, block)
    sent = kernel(
        begin, [(peers, block, count)],
        *[pltpu.with_memory_space_constraint(a, pltpu.HBM) for a in (strip, wanted, paired, own_inverse)],
        distant=4,
        scratch=(
            pltpu.VMEM((panel, window), jnp.float32),
            pltpu.VMEM((1, count), jnp.int32),
            pltpu.VMEM((1, count), jnp.int32),
            pltpu.VMEM((1, panel, block), jnp.float32),
            pltpu.SemaphoreType.DMA((4,)),
        ),
    )
    pieces = exchanged(sent, ROWS)
    early = kernel(opening, [(panel, count)], core, wanted, paired, strip, scalars=1)
    inverse = lax.all_gather(panel_inverse[0].reshape(-1, block), CORE)
    triangle = lax.all_gather(schur[: row_blocks // 2].reshape(-1, block), CORE)
    low = lax.all_gather(zslab[: zrow_blocks // 2].reshape(-1, block), CORE)
    high = lax.all_gather(zslab[zrow_blocks // 2 :].reshape(-1, block), CORE)
    pieces, early, inverse, triangle, low, high = lax.optimization_barrier(
        (pieces, early, inverse, triangle, low, high)
    )
    whole = lax.all_gather(jnp.sum(pieces, axis=0), CORE)
    partial_value, later = kernel(
        coupled, [(block, count), (block, count)], core, whole, triangle, scalars=1, block=block
    )
    parts = exchanged(partial_value.reshape(line, -1, count), LINE)
    mine = jnp.sum(parts, axis=0)
    summed = exchanged(jnp.broadcast_to(mine[None], (line, *mine.shape)), LINE).reshape(block, count)
    applied = kernel(solved, [(block, count)], summed, early, inverse, block=block)
    pieces = in_pairs(applied, ROWS[3], ROWS[:3])
    stacked = kernel(
        carried,
        [(line, zrow_blocks // 2, block // line, count)],
        pieces, later, low, high, block=block,
    )
    owned = jnp.sum(exchanged(stacked, LINE), axis=0)
    both = lax.all_gather(owned, CORE)
    squares = exchanged(kernel(squared, [(line, 1, count)], both), LINE)
    squares = exchanged(kernel(again, [(peers, 1, count)], squares), ROWS)
    total = zrow_blocks * block * peers
    rows = block // line // lax.axis_size(CORE)
    return kernel(
        finished, [(zrow_blocks, 1, rows, count)], core, both, squares, scalars=1, total=total
    )


def solution(mesh):
    split = Mesh(mesh.devices.reshape(2, 2, 2, 2, 16, 2), (*ROWS, *PCOL))
    placed = (
        P(None, ROWS, None, None, PCOL, None),
        P(None, PCOL, None, None, ROWS, None),
        P(None, ROWS, None, None),
        P(None, ROWS, None, None, PCOL, None),
        P(),
        P(),
    )
    return jax.shard_map(
        shards, mesh=split, in_specs=placed, out_specs=P(None, ROWS, PCOL, None), check_vma=False
    )
```

```python
import functools

import jax
import jax.numpy as jnp
from jax import lax
from jax.experimental import pallas as pl
from jax.experimental.pallas import tpu as pltpu
from jax.sharding import Mesh
from jax.sharding import PartitionSpec as P

ROWS = ("prow_0", "prow_1", "prow_2", "prow_3")
LINE = "pcol_0"
CORE = "pcol_1"
PCOL = (LINE, CORE)


EPSILON = 1e-06

FIRST = {"prow_0": 1, "prow_1": 0, "prow_2": 1, "prow_3": 0, "pcol_0": 8, "pcol_1": 0}


def product(left, right):
    return jnp.dot(left, right, precision=lax.Precision.HIGHEST, preferred_element_type=jnp.float32)


def in_turn(first, sizes):
    order = [0]
    for start, size in zip(first, sizes, strict=True):
        order = [place * size + (start + step) % size for place in order for step in range(size)]
    return [order]


def across_pairs():
    size = lax.axis_size(ROWS[2]) * lax.axis_size(ROWS[3])
    rows = lax.axis_size(ROWS[0]) * lax.axis_size(ROWS[1])
    first = rows // 2
    return [
        [(first + step) % rows * size + column for step in range(rows) for column in columns]
        for columns in ((2, 1), (3, 0))
    ]


def to_all_pairs(value):
    groups = across_pairs()
    sent = jnp.broadcast_to(value[None], (len(groups[0]), *value.shape))
    return lax.all_to_all(sent, ROWS, 0, 0, tiled=True, axis_index_groups=groups)


def exchanged(value, axis):
    names = (axis,) if isinstance(axis, str) else axis
    order = in_turn([FIRST[name] for name in names], [lax.axis_size(name) for name in names])
    return lax.all_to_all(value, axis, 0, 0, tiled=True, axis_index_groups=order)


def from_everyone(value, axis):
    size = lax.axis_size(axis)
    return exchanged(jnp.broadcast_to(value[None], (size, *value.shape)), axis)


def in_pairs(value, near):
    return to_all_pairs(jnp.sum(lax.all_gather(value, near), axis=0))


def first_half(shape):
    return lax.broadcasted_iota(jnp.int32, shape, 1) < shape[1] // 2


def turned(value):
    return pltpu.roll(value, value.shape[1] // 2, 1)


def doubled(value):
    left, other = first_half(value.shape), turned(value)
    return jnp.where(left, value, other), jnp.where(left, other, value)


def merged(low, high):
    return jnp.where(first_half(low.shape), low, high)


def strided(ref, core, start, count, step):
    return ref[core, pl.ds(start, count, stride=step), :]


def selected(targets_ref, flags_ref, window):
    lanes = targets_ref.shape[1]
    targets = targets_ref[...]
    columns = lax.broadcasted_iota(jnp.int32, (window, lanes), 0)
    flags = flags_ref[...].astype(jnp.float32)
    chosen = (columns == targets).astype(jnp.float32) + flags * (columns == targets + 1).astype(
        jnp.float32
    )
    return chosen.astype(jnp.bfloat16)


def thirds(value):
    high = value.astype(jnp.bfloat16)
    rest = value - high.astype(jnp.float32)
    middle = rest.astype(jnp.bfloat16)
    low = (rest - middle.astype(jnp.float32)).astype(jnp.bfloat16)
    return high, middle, low


def picked(parts, chosen):
    return sum(jnp.dot(part, chosen, preferred_element_type=jnp.float32) for part in reversed(parts))


def across(value, core):
    left, right = doubled(value)
    return jnp.where(core == 0, left, right)


def begin(
    strip_hbm, targets_hbm, flags_hbm, inverse_hbm,
    sent_ref, strip_ref, targets_ref, flags_ref, inverse_ref, sems,
):
    panel, window = strip_ref.shape
    block = sent_ref.shape[1]
    half = inverse_ref.shape[1]
    copies = [
        pltpu.make_async_copy(strip_hbm.at[pl.ds(panel, panel)], strip_ref, sems.at[0]),
        pltpu.make_async_copy(targets_hbm, targets_ref, sems.at[1]),
        pltpu.make_async_copy(flags_hbm, flags_ref, sems.at[2]),
        pltpu.make_async_copy(inverse_hbm.at[pl.ds(half, half)], inverse_ref.at[0], sems.at[3]),
    ]
    for copy in copies:
        copy.start()
    copies[1].wait()
    copies[2].wait()
    chosen = selected(targets_ref, flags_ref, window)
    copies[0].wait()
    late = -picked(thirds(strip_ref[...]), chosen)
    copies[3].wait()
    out = product(columns_of(inverse_ref, 0, 0, block), late)
    for peer in range(sent_ref.shape[0]):
        sent_ref[peer] = out


def columns_of(ref, core, start, count):
    return jnp.concatenate(
        [strided(ref, core, start, count, 2), strided(ref, core, start + 1, count, 2)], axis=1
    )


def opening(core_ref, targets_ref, flags_ref, strip_ref, early_ref):
    panel = strip_ref.shape[0] // 2
    chosen = selected(targets_ref, flags_ref, strip_ref.shape[1])
    early_ref[...] = across(-picked(thirds(strip_ref[:panel, :]), chosen), core_ref[0])


def coupled(core_ref, solved_ref, triangle_ref, sent_ref, later_ref, *, block):
    halves = [across(solved_ref[core], core_ref[0]) for core in range(2)]
    later_ref[...] = merged(*halves)
    both = jnp.concatenate(halves, axis=0)
    values = []
    for part in range(2):
        blocks = [strided(triangle_ref, core, part * 2 * block + 1, block, 2) for core in range(2)]
        values.append(product(jnp.concatenate(blocks, axis=1), both))
    sent_ref[...] = merged(*values)


def solved(summed_ref, early_ref, inverse_ref, sent_ref, *, block):
    residual = early_ref[...] - jnp.concatenate(doubled(summed_ref[...]), axis=0)
    sent_ref[...] = merged(
        *[product(columns_of(inverse_ref, core, 0, block), residual) for core in range(2)]
    )


def carried(pieces_ref, later_ref, low_ref, high_ref, sent_ref, *, block):
    sooner = doubled(jnp.sum(pieces_ref[...], axis=0))
    later = doubled(later_ref[...])
    known = [jnp.concatenate([sooner[core], later[core]], axis=0) for core in range(2)]
    values = []
    for ref in (low_ref, high_ref):
        rows = ref.shape[1] // 2
        values.append(sum(product(columns_of(ref, core, 0, rows), known[core]) for core in range(2)))
    out = merged(*values)
    peers, stacks, rows, lanes = sent_ref.shape
    first = FIRST[LINE]
    for stack in range(stacks):
        shares = out[stack * block : (stack + 1) * block].reshape(peers, rows, lanes)
        sent_ref[: peers - first, stack] = shares[first:]
        if first:
            sent_ref[peers - first :, stack] = shares[:first]


def squared(both_ref, sent_ref):
    both = both_ref[...]
    cores, stacks, rows, lanes = both.shape
    squares = jnp.sum((both * both).reshape(cores, stacks * rows, lanes), axis=1)
    squares = squares + turned(squares)
    out = merged(squares[0:1], squares[1:2])
    sent_ref[...] = jnp.broadcast_to(out[None], sent_ref.shape)


def again(pieces_ref, sent_ref):
    sent_ref[...] = jnp.broadcast_to(jnp.sum(pieces_ref[...], axis=0, keepdims=True), sent_ref.shape)


def finished(core_ref, both_ref, pieces_ref, out_ref, *, total):
    squares = jnp.sum(pieces_ref[...], axis=0)
    divisor = jnp.sqrt(squares / total + EPSILON)
    stacks = both_ref.shape[1]
    rows = out_ref.shape[2]
    for stack in range(stacks):
        low = both_ref[0, stack]
        high = both_ref[1, stack]
        for side, value in enumerate((merged(low, turned(high)), merged(turned(low), high))):
            value = value / divisor
            own = jnp.where(core_ref[0] == 0, value[:rows], value[rows:])
            out_ref[side * stacks + stack, 0] = own


LIMIT = 12 * 2**20
SCALAR = pl.BlockSpec(memory_space=pltpu.SMEM)
LOCAL = pl.BlockSpec(memory_space=pltpu.VMEM)
REMOTE = pl.BlockSpec(memory_space=pltpu.HBM)


def kernel(body, shapes, *args, scalars=0, distant=0, scratch=(), **settings):
    outs = [jax.ShapeDtypeStruct(shape, jnp.float32) for shape in shapes]
    single = len(outs) == 1
    return pl.pallas_call(
        functools.partial(body, **settings),
        out_shape=outs[0] if single else outs,
        in_specs=[SCALAR] * scalars + [LOCAL] * (len(args) - scalars - distant) + [REMOTE] * distant,
        out_specs=LOCAL if single else [LOCAL] * len(outs),
        scratch_shapes=list(scratch),
        name=body.__name__,
        compiler_params=pltpu.CompilerParams(vmem_limit_bytes=LIMIT),
    )(*args)


def shards(schur, panel_inverse, coupling, zslab, targets, pair_flags):
    block = schur.shape[2]
    row_blocks = schur.shape[0]
    window = coupling.shape[3]
    zrow_blocks = zslab.shape[0]
    count = targets.shape[0]
    line = lax.axis_size(LINE)
    peers = lax.axis_size(ROWS)
    panel = panel_inverse.shape[3] * block
    core = lax.axis_index(CORE).astype(jnp.int32).reshape(1)

    strip = coupling.reshape(row_blocks * block, window)
    wanted = targets.reshape(1, count)
    paired = pair_flags.reshape(1, count)
    own_inverse = panel_inverse.reshape(-1, block)
    sent = kernel(
        begin, [(peers, block, count)],
        *[pltpu.with_memory_space_constraint(a, pltpu.HBM) for a in (strip, wanted, paired, own_inverse)],
        distant=4,
        scratch=(
            pltpu.VMEM((panel, window), jnp.float32),
            pltpu.VMEM((1, count), jnp.int32),
            pltpu.VMEM((1, count), jnp.int32),
            pltpu.VMEM((1, panel, block), jnp.float32),
            pltpu.SemaphoreType.DMA((4,)),
        ),
    )
    pieces = exchanged(sent, ROWS)
    early = kernel(opening, [(panel, count)], core, wanted, paired, strip, scalars=1)
    inverse = lax.all_gather(panel_inverse[0].reshape(-1, block), CORE)
    triangle = lax.all_gather(schur[: row_blocks // 2].reshape(-1, block), CORE)
    low = lax.all_gather(zslab[: zrow_blocks // 2].reshape(-1, block), CORE)
    high = lax.all_gather(zslab[zrow_blocks // 2 :].reshape(-1, block), CORE)
    pieces, early, inverse, triangle, low, high = lax.optimization_barrier(
        (pieces, early, inverse, triangle, low, high)
    )
    whole = lax.all_gather(jnp.sum(pieces, axis=0), CORE)
    partial_value, later = kernel(
        coupled, [(block, count), (block, count)], core, whole, triangle, scalars=1, block=block
    )
    parts = exchanged(partial_value.reshape(line, -1, count), LINE)
    mine = jnp.sum(parts, axis=0)
    summed = exchanged(jnp.broadcast_to(mine[None], (line, *mine.shape)), LINE).reshape(block, count)
    applied = kernel(solved, [(block, count)], summed, early, inverse, block=block)
    pieces = in_pairs(applied, ROWS[3])
    stacked = kernel(
        carried,
        [(line, zrow_blocks // 2, block // line, count)],
        pieces, later, low, high, block=block,
    )
    owned = jnp.sum(exchanged(stacked, LINE), axis=0)
    both = lax.all_gather(owned, CORE)
    squares = exchanged(kernel(squared, [(line, 1, count)], both), LINE)
    squares = exchanged(kernel(again, [(peers, 1, count)], squares), ROWS)
    total = zrow_blocks * block * peers
    rows = block // line // lax.axis_size(CORE)
    return kernel(
        finished, [(zrow_blocks, 1, rows, count)], core, both, squares, scalars=1, total=total
    )


def solution(mesh):
    split = Mesh(mesh.devices.reshape(2, 2, 2, 2, 16, 2), (*ROWS, *PCOL))
    placed = (
        P(None, ROWS, None, None, PCOL, None),
        P(None, PCOL, None, None, ROWS, None),
        P(None, ROWS, None, None),
        P(None, ROWS, None, None, PCOL, None),
        P(),
        P(),
    )
    return jax.shard_map(
        shards, mesh=split, in_specs=placed, out_specs=P(None, ROWS, PCOL, None), check_vma=False
    )
```

```python
import functools

import jax
import jax.numpy as jnp
from jax import lax
from jax.experimental import pallas as pl
from jax.experimental.pallas import tpu as pltpu
from jax.sharding import Mesh
from jax.sharding import PartitionSpec as P

ROWS = ("prow_0", "prow_1", "prow_2", "prow_3")
LINE = "pcol_0"
CORE = "pcol_1"
PCOL = (LINE, CORE)


EPSILON = 1e-06

FIRST = {"prow_0": 1, "prow_1": 0, "prow_2": 1, "prow_3": 0, "pcol_0": 8, "pcol_1": 0}


def product(left, right):
    return jnp.dot(left, right, precision=lax.Precision.HIGHEST, preferred_element_type=jnp.float32)


def in_turn(first, sizes):
    order = [0]
    for start, size in zip(first, sizes, strict=True):
        order = [place * size + (start + step) % size for place in order for step in range(size)]
    return [order]


def across_pairs():
    size = lax.axis_size(ROWS[2]) * lax.axis_size(ROWS[3])
    rows = lax.axis_size(ROWS[0]) * lax.axis_size(ROWS[1])
    first = rows // 2
    return [
        [(first + step) % rows * size + column for step in range(rows) for column in columns]
        for columns in ((2, 1), (3, 0))
    ]


def to_all_pairs(value):
    groups = across_pairs()
    sent = jnp.broadcast_to(value[None], (len(groups[0]), *value.shape))
    return lax.all_to_all(sent, ROWS, 0, 0, tiled=True, axis_index_groups=groups)


def exchanged(value, axis):
    names = (axis,) if isinstance(axis, str) else axis
    order = in_turn([FIRST[name] for name in names], [lax.axis_size(name) for name in names])
    return lax.all_to_all(value, axis, 0, 0, tiled=True, axis_index_groups=order)


def from_everyone(value, axis):
    size = lax.axis_size(axis)
    return exchanged(jnp.broadcast_to(value[None], (size, *value.shape)), axis)


def in_pairs(value, near):
    return to_all_pairs(jnp.sum(lax.all_gather(value, near), axis=0))


def first_half(shape):
    return lax.broadcasted_iota(jnp.int32, shape, 1) < shape[1] // 2


def turned(value):
    return pltpu.roll(value, value.shape[1] // 2, 1)


def doubled(value):
    left, other = first_half(value.shape), turned(value)
    return jnp.where(left, value, other), jnp.where(left, other, value)


def merged(low, high):
    return jnp.where(first_half(low.shape), low, high)


def strided(ref, core, start, count, step):
    return ref[core, pl.ds(start, count, stride=step), :]


def selected(targets_ref, flags_ref, window):
    lanes = targets_ref.shape[1]
    targets = targets_ref[...]
    columns = lax.broadcasted_iota(jnp.int32, (window, lanes), 0)
    flags = flags_ref[...].astype(jnp.float32)
    chosen = (columns == targets).astype(jnp.float32) + flags * (columns == targets + 1).astype(
        jnp.float32
    )
    return chosen.astype(jnp.bfloat16)


def thirds(value):
    high = value.astype(jnp.bfloat16)
    rest = value - high.astype(jnp.float32)
    middle = rest.astype(jnp.bfloat16)
    low = (rest - middle.astype(jnp.float32)).astype(jnp.bfloat16)
    return high, middle, low


def picked(parts, chosen):
    return sum(jnp.dot(part, chosen, preferred_element_type=jnp.float32) for part in reversed(parts))


def folded(left, right):
    high, middle, low = [part.astype(jnp.float32) for part in thirds(right)]
    wide = jnp.concatenate([merged(high, middle), merged(low, jnp.zeros_like(low))], axis=1)
    total = picked(thirds(left), wide.astype(jnp.bfloat16))
    lanes = right.shape[1]
    parts = total[:, :lanes] + total[:, lanes:]
    return parts + turned(parts)


def across(value, core):
    left, right = doubled(value)
    return jnp.where(core == 0, left, right)


def begin(
    strip_hbm, targets_hbm, flags_hbm, inverse_hbm,
    sent_ref, strip_ref, targets_ref, flags_ref, inverse_ref, sems,
):
    panel, window = strip_ref.shape
    block = sent_ref.shape[1]
    half = inverse_ref.shape[1]
    copies = [
        pltpu.make_async_copy(strip_hbm.at[pl.ds(panel, panel)], strip_ref, sems.at[0]),
        pltpu.make_async_copy(targets_hbm, targets_ref, sems.at[1]),
        pltpu.make_async_copy(flags_hbm, flags_ref, sems.at[2]),
        pltpu.make_async_copy(inverse_hbm.at[pl.ds(half, half)], inverse_ref.at[0], sems.at[3]),
    ]
    for copy in copies:
        copy.start()
    copies[1].wait()
    copies[2].wait()
    chosen = selected(targets_ref, flags_ref, window)
    copies[0].wait()
    late = -picked(thirds(strip_ref[...]), chosen)
    copies[3].wait()
    out = product(columns_of(inverse_ref, 0, 0, block), late)
    for peer in range(sent_ref.shape[0]):
        sent_ref[peer] = out


def columns_of(ref, core, start, count):
    return jnp.concatenate(
        [strided(ref, core, start, count, 2), strided(ref, core, start + 1, count, 2)], axis=1
    )


def opening(core_ref, targets_ref, flags_ref, strip_ref, early_ref):
    panel = strip_ref.shape[0] // 2
    chosen = selected(targets_ref, flags_ref, strip_ref.shape[1])
    early_ref[...] = across(-picked(thirds(strip_ref[:panel, :]), chosen), core_ref[0])


def coupled(core_ref, solved_ref, triangle_ref, sent_ref, later_ref, *, block):
    halves = [across(solved_ref[core], core_ref[0]) for core in range(2)]
    later_ref[...] = merged(*halves)
    both = jnp.concatenate(halves, axis=0)
    values = []
    for part in range(2):
        blocks = [strided(triangle_ref, core, part * 2 * block + 1, block, 2) for core in range(2)]
        values.append(folded(jnp.concatenate(blocks, axis=1), both))
    sent_ref[...] = merged(*values)


def solved(summed_ref, early_ref, inverse_ref, sent_ref, *, block):
    residual = early_ref[...] - jnp.concatenate(doubled(summed_ref[...]), axis=0)
    sent_ref[...] = merged(
        *[folded(columns_of(inverse_ref, core, 0, block), residual) for core in range(2)]
    )


def carried(pieces_ref, later_ref, low_ref, high_ref, sent_ref, *, block):
    sooner = doubled(jnp.sum(pieces_ref[...], axis=0))
    later = doubled(later_ref[...])
    known = [jnp.concatenate([sooner[core], later[core]], axis=0) for core in range(2)]
    values = []
    for ref in (low_ref, high_ref):
        rows = ref.shape[1] // 2
        blocks = [columns_of(ref, core, 0, rows) for core in range(2)]
        values.append(folded(jnp.concatenate(blocks, axis=1), jnp.concatenate(known, axis=0)))
    out = merged(*values)
    peers, stacks, rows, lanes = sent_ref.shape
    first = FIRST[LINE]
    for stack in range(stacks):
        shares = out[stack * block : (stack + 1) * block].reshape(peers, rows, lanes)
        sent_ref[: peers - first, stack] = shares[first:]
        if first:
            sent_ref[peers - first :, stack] = shares[:first]


def squared(both_ref, sent_ref):
    both = both_ref[...]
    cores, stacks, rows, lanes = both.shape
    squares = jnp.sum((both * both).reshape(cores, stacks * rows, lanes), axis=1)
    squares = squares + turned(squares)
    out = merged(squares[0:1], squares[1:2])
    sent_ref[...] = jnp.broadcast_to(out[None], sent_ref.shape)


def again(pieces_ref, sent_ref):
    sent_ref[...] = jnp.broadcast_to(jnp.sum(pieces_ref[...], axis=0, keepdims=True), sent_ref.shape)


def finished(core_ref, both_ref, pieces_ref, out_ref, *, total):
    squares = jnp.sum(pieces_ref[...], axis=0)
    divisor = jnp.sqrt(squares / total + EPSILON)
    stacks = both_ref.shape[1]
    rows = out_ref.shape[2]
    for stack in range(stacks):
        low = both_ref[0, stack]
        high = both_ref[1, stack]
        for side, value in enumerate((merged(low, turned(high)), merged(turned(low), high))):
            value = value / divisor
            own = jnp.where(core_ref[0] == 0, value[:rows], value[rows:])
            out_ref[side * stacks + stack, 0] = own


LIMIT = 12 * 2**20
SCALAR = pl.BlockSpec(memory_space=pltpu.SMEM)
LOCAL = pl.BlockSpec(memory_space=pltpu.VMEM)
REMOTE = pl.BlockSpec(memory_space=pltpu.HBM)


def kernel(body, shapes, *args, scalars=0, distant=0, scratch=(), **settings):
    outs = [jax.ShapeDtypeStruct(shape, jnp.float32) for shape in shapes]
    single = len(outs) == 1
    return pl.pallas_call(
        functools.partial(body, **settings),
        out_shape=outs[0] if single else outs,
        in_specs=[SCALAR] * scalars + [LOCAL] * (len(args) - scalars - distant) + [REMOTE] * distant,
        out_specs=LOCAL if single else [LOCAL] * len(outs),
        scratch_shapes=list(scratch),
        name=body.__name__,
        compiler_params=pltpu.CompilerParams(vmem_limit_bytes=LIMIT),
    )(*args)


def shards(schur, panel_inverse, coupling, zslab, targets, pair_flags):
    block = schur.shape[2]
    row_blocks = schur.shape[0]
    window = coupling.shape[3]
    zrow_blocks = zslab.shape[0]
    count = targets.shape[0]
    line = lax.axis_size(LINE)
    peers = lax.axis_size(ROWS)
    panel = panel_inverse.shape[3] * block
    core = lax.axis_index(CORE).astype(jnp.int32).reshape(1)

    strip = coupling.reshape(row_blocks * block, window)
    wanted = targets.reshape(1, count)
    paired = pair_flags.reshape(1, count)
    own_inverse = panel_inverse.reshape(-1, block)
    sent = kernel(
        begin, [(peers, block, count)],
        *[pltpu.with_memory_space_constraint(a, pltpu.HBM) for a in (strip, wanted, paired, own_inverse)],
        distant=4,
        scratch=(
            pltpu.VMEM((panel, window), jnp.float32),
            pltpu.VMEM((1, count), jnp.int32),
            pltpu.VMEM((1, count), jnp.int32),
            pltpu.VMEM((1, panel, block), jnp.float32),
            pltpu.SemaphoreType.DMA((4,)),
        ),
    )
    pieces = exchanged(sent, ROWS)
    early = kernel(opening, [(panel, count)], core, wanted, paired, strip, scalars=1)
    inverse = lax.all_gather(panel_inverse[0].reshape(-1, block), CORE)
    triangle = lax.all_gather(schur[: row_blocks // 2].reshape(-1, block), CORE)
    low = lax.all_gather(zslab[: zrow_blocks // 2].reshape(-1, block), CORE)
    high = lax.all_gather(zslab[zrow_blocks // 2 :].reshape(-1, block), CORE)
    pieces, early, inverse, triangle, low, high = lax.optimization_barrier(
        (pieces, early, inverse, triangle, low, high)
    )
    whole = lax.all_gather(jnp.sum(pieces, axis=0), CORE)
    partial_value, later = kernel(
        coupled, [(block, count), (block, count)], core, whole, triangle, scalars=1, block=block
    )
    parts = exchanged(partial_value.reshape(line, -1, count), LINE)
    mine = jnp.sum(parts, axis=0)
    summed = exchanged(jnp.broadcast_to(mine[None], (line, *mine.shape)), LINE).reshape(block, count)
    applied = kernel(solved, [(block, count)], summed, early, inverse, block=block)
    pieces = in_pairs(applied, ROWS[3])
    stacked = kernel(
        carried,
        [(line, zrow_blocks // 2, block // line, count)],
        pieces, later, low, high, block=block,
    )
    owned = jnp.sum(exchanged(stacked, LINE), axis=0)
    both = lax.all_gather(owned, CORE)
    squares = exchanged(kernel(squared, [(line, 1, count)], both), LINE)
    squares = exchanged(kernel(again, [(peers, 1, count)], squares), ROWS)
    total = zrow_blocks * block * peers
    rows = block // line // lax.axis_size(CORE)
    return kernel(
        finished, [(zrow_blocks, 1, rows, count)], core, both, squares, scalars=1, total=total
    )


def solution(mesh):
    split = Mesh(mesh.devices.reshape(2, 2, 2, 2, 16, 2), (*ROWS, *PCOL))
    placed = (
        P(None, ROWS, None, None, PCOL, None),
        P(None, PCOL, None, None, ROWS, None),
        P(None, ROWS, None, None),
        P(None, ROWS, None, None, PCOL, None),
        P(),
        P(),
    )
    return jax.shard_map(
        shards, mesh=split, in_specs=placed, out_specs=P(None, ROWS, PCOL, None), check_vma=False
    )
```

```python
import functools

import jax
import jax.numpy as jnp
from jax import lax
from jax.experimental import pallas as pl
from jax.experimental.pallas import tpu as pltpu
from jax.sharding import Mesh
from jax.sharding import PartitionSpec as P

ROWS = ("prow_0", "prow_1", "prow_2", "prow_3")
LINE = "pcol_0"
CORE = "pcol_1"
PCOL = (LINE, CORE)


EPSILON = 1e-06

FIRST = {"prow_0": 1, "prow_1": 0, "prow_2": 1, "prow_3": 0, "pcol_0": 9, "pcol_1": 0}


def product(left, right):
    return jnp.dot(left, right, precision=lax.Precision.HIGHEST, preferred_element_type=jnp.float32)


def in_turn(first, sizes):
    order = [0]
    for start, size in zip(first, sizes, strict=True):
        order = [place * size + (start + step) % size for place in order for step in range(size)]
    return [order]


def across_pairs():
    size = lax.axis_size(ROWS[2]) * lax.axis_size(ROWS[3])
    rows = lax.axis_size(ROWS[0]) * lax.axis_size(ROWS[1])
    first = rows // 2
    return [
        [(first + step) % rows * size + column for step in range(rows) for column in columns]
        for columns in ((2, 1), (3, 0))
    ]


def to_all_pairs(value):
    groups = across_pairs()
    sent = jnp.broadcast_to(value[None], (len(groups[0]), *value.shape))
    return lax.all_to_all(sent, ROWS, 0, 0, tiled=True, axis_index_groups=groups)


def exchanged(value, axis):
    names = (axis,) if isinstance(axis, str) else axis
    order = in_turn([FIRST[name] for name in names], [lax.axis_size(name) for name in names])
    return lax.all_to_all(value, axis, 0, 0, tiled=True, axis_index_groups=order)


def from_everyone(value, axis):
    size = lax.axis_size(axis)
    return exchanged(jnp.broadcast_to(value[None], (size, *value.shape)), axis)


def in_pairs(value, near):
    return to_all_pairs(jnp.sum(lax.all_gather(value, near), axis=0))


def first_half(shape):
    return lax.broadcasted_iota(jnp.int32, shape, 1) < shape[1] // 2


def turned(value):
    return pltpu.roll(value, value.shape[1] // 2, 1)


def doubled(value):
    left, other = first_half(value.shape), turned(value)
    return jnp.where(left, value, other), jnp.where(left, other, value)


def merged(low, high):
    return jnp.where(first_half(low.shape), low, high)


def strided(ref, core, start, count, step):
    return ref[core, pl.ds(start, count, stride=step), :]


def selected(targets_ref, flags_ref, window):
    lanes = targets_ref.shape[1]
    targets = targets_ref[...]
    columns = lax.broadcasted_iota(jnp.int32, (window, lanes), 0)
    flags = flags_ref[...].astype(jnp.float32)
    chosen = (columns == targets).astype(jnp.float32) + flags * (columns == targets + 1).astype(
        jnp.float32
    )
    return chosen.astype(jnp.bfloat16)


def thirds(value):
    high = value.astype(jnp.bfloat16)
    rest = value - high.astype(jnp.float32)
    middle = rest.astype(jnp.bfloat16)
    low = (rest - middle.astype(jnp.float32)).astype(jnp.bfloat16)
    return high, middle, low


def picked(parts, chosen):
    return sum(jnp.dot(part, chosen, preferred_element_type=jnp.float32) for part in reversed(parts))


def folded(left, right):
    high, middle, low = [part.astype(jnp.float32) for part in thirds(right)]
    wide = jnp.concatenate([merged(high, middle), merged(low, jnp.zeros_like(low))], axis=1)
    total = picked(thirds(left), wide.astype(jnp.bfloat16))
    lanes = right.shape[1]
    parts = total[:, :lanes] + total[:, lanes:]
    return parts + turned(parts)


def across(value, core):
    left, right = doubled(value)
    return jnp.where(core == 0, left, right)


def begin(
    strip_hbm, targets_hbm, flags_hbm, inverse_hbm,
    sent_ref, strip_ref, targets_ref, flags_ref, inverse_ref, sems,
):
    panel, window = strip_ref.shape
    block = sent_ref.shape[0]
    half = inverse_ref.shape[1]
    copies = [
        pltpu.make_async_copy(strip_hbm.at[pl.ds(panel, panel)], strip_ref, sems.at[0]),
        pltpu.make_async_copy(targets_hbm, targets_ref, sems.at[1]),
        pltpu.make_async_copy(flags_hbm, flags_ref, sems.at[2]),
        pltpu.make_async_copy(inverse_hbm.at[pl.ds(half, half)], inverse_ref.at[0], sems.at[3]),
    ]
    for copy in copies:
        copy.start()
    copies[1].wait()
    copies[2].wait()
    chosen = selected(targets_ref, flags_ref, window)
    copies[0].wait()
    late = -picked(thirds(strip_ref[...]), chosen)
    copies[3].wait()
    sent_ref[...] = product(columns_of(inverse_ref, 0, 0, block), late)


def columns_of(ref, core, start, count):
    return jnp.concatenate(
        [strided(ref, core, start, count, 2), strided(ref, core, start + 1, count, 2)], axis=1
    )


def opening(core_ref, targets_ref, flags_ref, strip_ref, early_ref):
    panel = strip_ref.shape[0] // 2
    chosen = selected(targets_ref, flags_ref, strip_ref.shape[1])
    early_ref[...] = across(-picked(thirds(strip_ref[:panel, :]), chosen), core_ref[0])


def mixed(core_ref, near_ref, sent_ref):
    sums = [near_ref[core] + near_ref[2 + core] for core in range(2)]
    out = merged(*[across(value, core_ref[0]) for value in sums])
    for peer in range(sent_ref.shape[0]):
        sent_ref[peer] = out


def coupled(pieces_ref, triangle_ref, sent_ref, later_ref, *, block):
    later = jnp.sum(pieces_ref[...], axis=0)
    later_ref[...] = later
    halves = doubled(later)
    both = jnp.concatenate(halves, axis=0)
    values = []
    for part in range(2):
        blocks = [strided(triangle_ref, core, part * 2 * block + 1, block, 2) for core in range(2)]
        values.append(folded(jnp.concatenate(blocks, axis=1), both))
    sent_ref[...] = merged(*values)


def solved(summed_ref, early_ref, inverse_ref, sent_ref, *, block):
    residual = early_ref[...] - jnp.concatenate(doubled(summed_ref[...]), axis=0)
    sent_ref[...] = merged(
        *[folded(columns_of(inverse_ref, core, 0, block), residual) for core in range(2)]
    )


def carried(pieces_ref, later_ref, low_ref, high_ref, sent_ref, *, block):
    sooner = doubled(jnp.sum(pieces_ref[...], axis=0))
    later = doubled(later_ref[...])
    known = [jnp.concatenate([sooner[core], later[core]], axis=0) for core in range(2)]
    values = []
    for ref in (low_ref, high_ref):
        rows = ref.shape[1] // 2
        blocks = [columns_of(ref, core, 0, rows) for core in range(2)]
        values.append(folded(jnp.concatenate(blocks, axis=1), jnp.concatenate(known, axis=0)))
    out = merged(*values)
    peers, stacks, rows, lanes = sent_ref.shape
    first = FIRST[LINE]
    for stack in range(stacks):
        shares = out[stack * block : (stack + 1) * block].reshape(peers, rows, lanes)
        sent_ref[: peers - first, stack] = shares[first:]
        if first:
            sent_ref[peers - first :, stack] = shares[:first]


def squared(both_ref, sent_ref):
    both = both_ref[...]
    cores, stacks, rows, lanes = both.shape
    squares = jnp.sum((both * both).reshape(cores, stacks * rows, lanes), axis=1)
    squares = squares + turned(squares)
    out = merged(squares[0:1], squares[1:2])
    sent_ref[...] = jnp.broadcast_to(out[None], sent_ref.shape)


def again(pieces_ref, sent_ref):
    sent_ref[...] = jnp.broadcast_to(jnp.sum(pieces_ref[...], axis=0, keepdims=True), sent_ref.shape)


def finished(core_ref, both_ref, pieces_ref, out_ref, *, total):
    squares = jnp.sum(pieces_ref[...], axis=0)
    divisor = jnp.sqrt(squares / total + EPSILON)
    stacks = both_ref.shape[1]
    rows = out_ref.shape[2]
    for stack in range(stacks):
        low = both_ref[0, stack]
        high = both_ref[1, stack]
        for side, value in enumerate((merged(low, turned(high)), merged(turned(low), high))):
            value = value / divisor
            own = jnp.where(core_ref[0] == 0, value[:rows], value[rows:])
            out_ref[side * stacks + stack, 0] = own


LIMIT = 12 * 2**20
SCALAR = pl.BlockSpec(memory_space=pltpu.SMEM)
LOCAL = pl.BlockSpec(memory_space=pltpu.VMEM)
REMOTE = pl.BlockSpec(memory_space=pltpu.HBM)


def kernel(body, shapes, *args, scalars=0, distant=0, scratch=(), **settings):
    outs = [jax.ShapeDtypeStruct(shape, jnp.float32) for shape in shapes]
    single = len(outs) == 1
    return pl.pallas_call(
        functools.partial(body, **settings),
        out_shape=outs[0] if single else outs,
        in_specs=[SCALAR] * scalars + [LOCAL] * (len(args) - scalars - distant) + [REMOTE] * distant,
        out_specs=LOCAL if single else [LOCAL] * len(outs),
        scratch_shapes=list(scratch),
        name=body.__name__,
        compiler_params=pltpu.CompilerParams(vmem_limit_bytes=LIMIT),
    )(*args)


def shards(schur, panel_inverse, coupling, zslab, targets, pair_flags):
    block = schur.shape[2]
    row_blocks = schur.shape[0]
    window = coupling.shape[3]
    zrow_blocks = zslab.shape[0]
    count = targets.shape[0]
    line = lax.axis_size(LINE)
    peers = lax.axis_size(ROWS)
    panel = panel_inverse.shape[3] * block
    core = lax.axis_index(CORE).astype(jnp.int32).reshape(1)

    strip = coupling.reshape(row_blocks * block, window)
    wanted = targets.reshape(1, count)
    paired = pair_flags.reshape(1, count)
    own_inverse = panel_inverse.reshape(-1, block)
    sent = kernel(
        begin, [(block, count)],
        *[pltpu.with_memory_space_constraint(a, pltpu.HBM) for a in (strip, wanted, paired, own_inverse)],
        distant=4,
        scratch=(
            pltpu.VMEM((panel, window), jnp.float32),
            pltpu.VMEM((1, count), jnp.int32),
            pltpu.VMEM((1, count), jnp.int32),
            pltpu.VMEM((1, panel, block), jnp.float32),
            pltpu.SemaphoreType.DMA((4,)),
        ),
    )
    near = lax.all_gather(sent, (ROWS[3], CORE))
    pieces = lax.all_to_all(
        kernel(mixed, [(peers // 2, block, count)], core, near, scalars=1),
        ROWS, 0, 0, tiled=True, axis_index_groups=across_pairs(),
    )
    early = kernel(opening, [(panel, count)], core, wanted, paired, strip, scalars=1)
    inverse = lax.all_gather(panel_inverse[0].reshape(-1, block), CORE)
    triangle = lax.all_gather(schur[: row_blocks // 2].reshape(-1, block), CORE)
    pieces, early, inverse, triangle, zslab = lax.optimization_barrier(
        (pieces, early, inverse, triangle, zslab)
    )
    partial_value, later = kernel(
        coupled, [(block, count), (block, count)], pieces, triangle, block=block
    )
    parts = exchanged(partial_value.reshape(line, -1, count), LINE)
    low = lax.all_gather(zslab[: zrow_blocks // 2].reshape(-1, block), CORE)
    high = lax.all_gather(zslab[zrow_blocks // 2 :].reshape(-1, block), CORE)
    parts, low, high = lax.optimization_barrier(
        (parts, low, high)
    )
    mine = jnp.sum(parts, axis=0)
    summed = exchanged(jnp.broadcast_to(mine[None], (line, *mine.shape)), LINE).reshape(block, count)
    applied = kernel(solved, [(block, count)], summed, early, inverse, block=block)
    pieces = in_pairs(applied, ROWS[3])
    stacked = kernel(
        carried,
        [(line, zrow_blocks // 2, block // line, count)],
        pieces, later, low, high, block=block,
    )
    owned = jnp.sum(exchanged(stacked, LINE), axis=0)
    both = lax.all_gather(owned, CORE)
    squares = exchanged(kernel(squared, [(line, 1, count)], both), LINE)
    squares = exchanged(kernel(again, [(peers, 1, count)], squares), ROWS)
    total = zrow_blocks * block * peers
    rows = block // line // lax.axis_size(CORE)
    return kernel(
        finished, [(zrow_blocks, 1, rows, count)], core, both, squares, scalars=1, total=total
    )


def solution(mesh):
    split = Mesh(mesh.devices.reshape(2, 2, 2, 2, 16, 2), (*ROWS, *PCOL))
    placed = (
        P(None, ROWS, None, None, PCOL, None),
        P(None, PCOL, None, None, ROWS, None),
        P(None, ROWS, None, None),
        P(None, ROWS, None, None, PCOL, None),
        P(),
        P(),
    )
    return jax.shard_map(
        shards, mesh=split, in_specs=placed, out_specs=P(None, ROWS, PCOL, None), check_vma=False
    )
```
